32 devices in a mesh: blk: 8 (over z, x), grp: 4 (over y, core).
Axes of the slice: x: 2, y: 2, z: 4, core: 2. Of those that a mesh axis runs over, the one named last changes fastest.
Arguments:
- query_rows: bfloat16 [4096, 128], P(('blk', 'grp')), may hold values from -36 to 36
- key_rows: bfloat16 [4096, 128], P(('blk', 'grp')), may hold values from -6 to 6
- value_rows: bfloat16 [4096, 128], P(('blk', 'grp')), may hold values from -6 to 6
- query_tangent: bfloat16 [4096, 128], P(('blk', 'grp')), may hold values from -6 to 6
- key_tangent: bfloat16 [4096, 128], P(('blk', 'grp')), may hold values from -6 to 6
- value_tangent: bfloat16 [4096, 128], P(('blk', 'grp')), may hold values from -6 to 6
Outputs:
- attended: float32 [4096, 128], P(('blk', 'grp'))
- tangent_out: float32 [4096, 128], P(('blk', 'grp'))
The draws below stay inside these ranges and needn't reach their ends.
All inputs are finite; a program needn't handle non-finite values.
Results may differ from the reference program's by a relative error of at most 0.02.
Values may be sent and summed in bfloat16 or wider, within the bound.
No kernel may reach another device: no remote copies, remote signals or barrier semaphores. Data moves between devices by JAX's collectives and lax.ppermute only.
A program may use at most 128 MiB of HBM per device.

```python
import math
import jax
import jax.numpy as jnp
from jax import lax

HD = 128
TOK_DEV = 128
SEQ = 4096
N_GRP = 4


def draw_query_rows(key, part):
    noise_key = jax.random.fold_in(key, 1)
    scale_key = jax.random.fold_in(key, 2)
    noise_field = jax.random.truncated_normal(noise_key, -6.0, 6.0, (SEQ, HD), jnp.float32)
    row_scale = jnp.exp(jax.random.uniform(scale_key, (SEQ, 1), jnp.float32, 0.0, math.log(6.0)))
    result = noise_field * row_scale
    return result.astype(jnp.bfloat16)


def draw_key_rows(key, part):
    noise_key = jax.random.fold_in(key, 3)
    result = jax.random.truncated_normal(noise_key, -6.0, 6.0, (SEQ, HD), jnp.float32)
    return result.astype(jnp.bfloat16)


def level_of(rng, shape, split, least, high):
    gain = 1.0
    for axis_at, parts in split:
        steps = jax.random.uniform(jax.random.fold_in(jax.random.fold_in(rng, 6), axis_at), (parts,), jnp.float32, least / len(split), high / len(split))
        gain = gain * jnp.repeat(jnp.exp(steps), shape[axis_at] // parts).reshape((-1,) + (1,) * (len(shape) - 1 - axis_at))
    return gain


def centred(key, dims, deviation, reach, cuts=(), kind=jnp.bfloat16):
    values = jax.random.normal(key, dims, jnp.float32) * deviation
    if len(cuts) > 0:
        values = level_of(key, dims, cuts, -0.22, 0.18) * values
    return jnp.clip(values, min=-reach, max=reach).astype(kind)


def setup_inputs(seed: int = 0) -> dict:
    streams_of = jax.random.split(jax.random.key(seed), 7)
    return {
        "query_rows": draw_query_rows(jax.random.fold_in(streams_of[6], 71), 0),
        "key_rows": draw_key_rows(jax.random.fold_in(streams_of[6], 71), 0),
        "value_rows": centred(streams_of[2], (SEQ, HD), 1.0, 6.0, ((0, 32),)),
        "query_tangent": centred(streams_of[3], (SEQ, HD), 1.0, 6.0, ((0, 32),)),
        "key_tangent": centred(streams_of[4], (SEQ, HD), 1.0, 6.0, ((0, 32),)),
        "value_tangent": centred(streams_of[5], (SEQ, HD), 1.0, 6.0, ((0, 32),)),
    }


def reference(query_rows, key_rows, value_rows, query_tangent, key_tangent, value_tangent):
    score_scale = HD ** -0.5
    span_rows = TOK_DEV * N_GRP

    def one_panel(pieces):
        query_part, tangent_part = pieces
        scores = jnp.dot(query_part, key_rows.T, preferred_element_type=jnp.float32) * score_scale
        slopes = (jnp.dot(tangent_part, key_rows.T, preferred_element_type=jnp.float32)
                  + jnp.dot(query_part, key_tangent.T, preferred_element_type=jnp.float32)) * score_scale
        row_max = jnp.max(scores, axis=1, keepdims=True)
        probs = jnp.exp(scores - row_max)
        row_total = jnp.sum(probs, axis=1, keepdims=True)
        weighted = probs * slopes
        slope_total = jnp.sum(weighted, axis=1, keepdims=True)
        probs_low = probs.astype(jnp.bfloat16)
        weighted_low = weighted.astype(jnp.bfloat16)
        primal_sum = jnp.dot(probs_low, value_rows, preferred_element_type=jnp.float32)
        tangent_sum = (jnp.dot(probs_low, value_tangent, preferred_element_type=jnp.float32)
                       + jnp.dot(weighted_low, value_rows, preferred_element_type=jnp.float32))
        attended = primal_sum / row_total
        tangent_out = tangent_sum / row_total - (slope_total / row_total) * attended
        return attended, tangent_out

    shaped = (query_rows.reshape(SEQ // span_rows, span_rows, HD),
              query_tangent.reshape(SEQ // span_rows, span_rows, HD))
    attended, tangent_out = lax.map(one_panel, shaped)
    return attended.reshape(SEQ, HD), tangent_out.reshape(SEQ, HD)
```

```python
import functools

import jax
import jax.numpy as jnp
from jax import lax
from jax.experimental import pallas as pl
from jax.experimental.pallas import tpu as pltpu
from jax.sharding import PartitionSpec as P


TAIL = 16
VMEM = pl.BlockSpec(memory_space=pltpu.VMEM)


def split3(x):
    hi = x.astype(jnp.bfloat16).astype(jnp.float32)
    mid = (x - hi).astype(jnp.bfloat16).astype(jnp.float32)
    return hi, mid, x - hi - mid


def panel_kernel(count, scale, q_ref, near_ref, far_ref, own_ref, stat_ref, *send_refs):
    rows, width = own_ref.shape
    head = width // 2
    nt = (((1,), (1,)), ((), ()))
    nn = (((1,), (0,)), ((), ()))
    f32 = jnp.float32
    lane = lax.broadcasted_iota(jnp.int32, (rows, head), 1)
    for block in range(count):
        q = q_ref[block * rows : (block + 1) * rows, :]
        primal_q = q[:, head:]
        scores = [
            lax.dot_general(primal_q, kv[:, :head], nt, preferred_element_type=f32)
            for kv in (near_ref, far_ref)
        ]
        slopes = [
            lax.dot_general(q, kv[:, :width], nt, preferred_element_type=f32)
            for kv in (near_ref, far_ref)
        ]
        top = functools.reduce(
            jnp.maximum, [jnp.max(s, axis=1, keepdims=True) for s in scores]
        )
        total = slope_total = both = slope_part = None
        for s, d, kv in zip(scores, slopes, (near_ref, far_ref)):
            probs = jnp.exp((s - top) * scale)
            weighted = probs * d
            a = jnp.sum(probs, axis=1, keepdims=True)
            b = jnp.sum(weighted, axis=1, keepdims=True)
            c = lax.dot_general(
                probs.astype(jnp.bfloat16), kv[:, width:], nn, preferred_element_type=f32
            )
            e = lax.dot_general(
                weighted.astype(jnp.bfloat16),
                kv[:, width : width + head],
                nn,
                preferred_element_type=f32,
            )
            if total is None:
                total, slope_total, both, slope_part = a, b, c, e
            else:
                total, slope_total = total + a, slope_total + b
                both, slope_part = both + c, slope_part + e
        inverse = 1.0 / total
        attended = both[:, :head] * inverse
        slope_mean = slope_total * (scale * inverse)
        tangent = (both[:, head:] + slope_part * scale) * inverse - slope_mean * attended
        lse = top * scale + jnp.log(total)
        if block == 0:
            own_ref[:, :head] = attended
            own_ref[:, head:] = tangent
            stat_ref[...] = jnp.where(lane == 0, lse, slope_mean)
        else:
            out = send_refs[block - 1]
            out[:rows, :head] = attended.astype(jnp.bfloat16)
            out[:rows, head:] = tangent.astype(jnp.bfloat16)
            pieces = split3(lse) + split3(slope_mean)
            tile = jnp.zeros((rows, head), f32)
            for at, piece in enumerate(pieces):
                tile = jnp.where(lane == at, piece, tile)
            out[rows:, :head] = tile.T[:TAIL, :].astype(jnp.bfloat16)
            out[rows:, head:] = jnp.zeros((TAIL, head), jnp.bfloat16)


def merge_kernel(own_ref, stat_ref, *refs):
    got_refs, (attended_ref, tangent_ref) = refs[:-2], refs[-2:]
    rows, head = attended_ref.shape
    f32 = jnp.float32
    parts = [(own_ref[:, :head], own_ref[:, head:], stat_ref[:, 0:1], stat_ref[:, 1:2])]
    for got in got_refs:
        cols = got[rows:, :head].astype(f32).T
        parts.append(
            (
                got[:rows, :head].astype(f32),
                got[:rows, head:].astype(f32),
                cols[:, 0:1] + cols[:, 1:2] + cols[:, 2:3],
                cols[:, 3:4] + cols[:, 4:5] + cols[:, 5:6],
            )
        )
    top = functools.reduce(jnp.maximum, [p[2] for p in parts])
    weights = [jnp.exp(p[2] - top) for p in parts]
    inverse = 1.0 / sum(weights)
    weights = [w * inverse for w in weights]
    mean = sum(w * p[3] for w, p in zip(weights, parts))
    attended_ref[...] = sum(w * p[0] for w, p in zip(weights, parts))
    tangent_ref[...] = sum(
        w * p[1] + (w * (p[3] - mean)) * p[0] for w, p in zip(weights, parts)
    )


def on_device(shape, query_rows, key_rows, value_rows, query_tangent, key_tangent, value_tangent):
    outer, inner, side, cores = shape
    plane = inner * side
    rows, head = query_rows.shape
    scale = head ** (-0.5)
    axes = ("blk", "grp")
    mix = lambda i, s, n: i ^ s if n & (n - 1) == 0 else (i + s) % n
    back = lambda i, s, n: i ^ s if n & (n - 1) == 0 else (i - s) % n

    def index(o, p, c):
        return (o * plane + p) * cores + c

    every = [(o, p, c) for o in range(outer) for p in range(plane) for c in range(cores)]
    over_plane = lambda s: [(index(o, p, c), index(o, mix(p, s, plane), c)) for o, p, c in every]
    over_core = [(index(o, p, c), index(o, p, (c + 1) % cores)) for o, p, c in every]
    over_outer = lambda s: [(index(o, p, c), index(mix(o, s, outer), p, c)) for o, p, c in every]
    outer_back = lambda s: [(index(o, p, c), index(back(o, s, outer), p, c)) for o, p, c in every]

    kv = jnp.concatenate([key_rows, key_tangent, value_rows, value_tangent], axis=1)
    q = jnp.concatenate([query_tangent, query_rows], axis=1)
    near = jnp.concatenate(
        [kv] + [lax.ppermute(kv, axes, over_plane(s)) for s in range(1, plane)], axis=0
    )
    queries = jnp.concatenate(
        [q] + [lax.ppermute(q, axes, over_outer(s)) for s in range(1, outer)], axis=0
    )
    far = lax.ppermute(near, axes, over_core)

    bf16, f32 = jnp.bfloat16, jnp.float32
    panel = pl.pallas_call(
        functools.partial(panel_kernel, outer, scale),
        out_shape=(
            jax.ShapeDtypeStruct((rows, 2 * head), f32),
            jax.ShapeDtypeStruct((rows, head), f32),
        )
        + tuple(jax.ShapeDtypeStruct((rows + TAIL, 2 * head), bf16) for _ in range(1, outer)),
        in_specs=[VMEM] * 3,
        out_specs=(VMEM,) * (1 + outer),
        compiler_params=pltpu.CompilerParams(vmem_limit_bytes=40 * 2**20),
        cost_estimate=pl.CostEstimate(
            flops=10 * queries.shape[0] * 2 * near.shape[0] * head,
            bytes_accessed=0,
            transcendentals=0,
        ),
        name="panel",
    )
    own, stat, *sends = panel(queries, near, far)
    gots = [
        lax.ppermute(block, axes, outer_back(s)) for s, block in zip(range(1, outer), sends)
    ]
    return pl.pallas_call(
        merge_kernel,
        out_shape=(jax.ShapeDtypeStruct((rows, head), f32),) * 2,
        in_specs=[VMEM] * (2 + len(gots)),
        out_specs=(VMEM, VMEM),
        compiler_params=pltpu.CompilerParams(vmem_limit_bytes=8 * 2**20),
        name="merge",
    )(own, stat, *gots)


def solution(mesh):
    blocks, group = mesh.shape["blk"], mesh.shape["grp"]
    cores = 2 if group % 2 == 0 else 1
    outer = group if blocks % group == 0 else 1
    shape = (outer, blocks // outer, group // cores, cores)
    placed = P(("blk", "grp"), None)
    return jax.shard_map(
        functools.partial(on_device, shape),
        mesh=mesh,
        in_specs=(placed,) * 6,
        out_specs=(placed, placed),
        check_vma=False,
    )
```

```python
import functools

import jax
import jax.numpy as jnp
from jax import lax
from jax.experimental import pallas as pl
from jax.experimental.pallas import tpu as pltpu
from jax.sharding import PartitionSpec as P


TAIL = 8
VMEM = pl.BlockSpec(memory_space=pltpu.VMEM)


def pack_kernel(k, dk, v, dv, q, dq, kv_out, q_out, sems):
    head = k.shape[1]
    places = [
        (k, kv_out, 0), (dk, kv_out, 1), (v, kv_out, 2), (dv, kv_out, 3),
        (dq, q_out, 0), (q, q_out, 1),
    ]
    copies = [
        pltpu.make_async_copy(src, out.at[:, at * head : (at + 1) * head], sems.at[i])
        for i, (src, out, at) in enumerate(places)
    ]
    for copy in copies:
        copy.start()
    for copy in copies:
        copy.wait()


def split3(x):
    hi = x.astype(jnp.bfloat16).astype(jnp.float32)
    mid = (x - hi).astype(jnp.bfloat16).astype(jnp.float32)
    return hi, mid, x - hi - mid


def panel_kernel(count, scale, q_ref, near_ref, far_ref, own_ref, stat_ref, *send_refs):
    rows, width = own_ref.shape
    head = width // 2
    nt = (((1,), (1,)), ((), ()))
    nn = (((1,), (0,)), ((), ()))
    f32 = jnp.float32
    lane = lax.broadcasted_iota(jnp.int32, (rows, head), 1)
    for block in range(count):
        q = q_ref[block * rows : (block + 1) * rows, :]
        primal_q = q[:, head:]
        scores = [
            lax.dot_general(primal_q, kv[:, :head], nt, preferred_element_type=f32)
            for kv in (near_ref, far_ref)
        ]
        slopes = [
            lax.dot_general(q, kv[:, :width], nt, preferred_element_type=f32)
            for kv in (near_ref, far_ref)
        ]
        top = functools.reduce(
            jnp.maximum, [jnp.max(s, axis=1, keepdims=True) for s in scores]
        )
        total = slope_total = both = slope_part = None
        for s, d, kv in zip(scores, slopes, (near_ref, far_ref)):
            probs = jnp.exp((s - top) * scale)
            weighted = probs * d
            a = jnp.sum(probs, axis=1, keepdims=True)
            b = jnp.sum(weighted, axis=1, keepdims=True)
            c = lax.dot_general(
                probs.astype(jnp.bfloat16), kv[:, width:], nn, preferred_element_type=f32
            )
            e = lax.dot_general(
                weighted.astype(jnp.bfloat16),
                kv[:, width : width + head],
                nn,
                preferred_element_type=f32,
            )
            if total is None:
                total, slope_total, both, slope_part = a, b, c, e
            else:
                total, slope_total = total + a, slope_total + b
                both, slope_part = both + c, slope_part + e
        inverse = 1.0 / total
        attended = both[:, :head] * inverse
        slope_mean = slope_total * (scale * inverse)
        tangent = (both[:, head:] + slope_part * scale) * inverse - slope_mean * attended
        lse = top * scale + jnp.log(total)
        if block == 0:
            own_ref[:, :head] = attended
            own_ref[:, head:] = tangent
            stat_ref[...] = jnp.where(lane == 0, lse, slope_mean)
        else:
            out = send_refs[block - 1]
            out[:rows, :head] = attended.astype(jnp.bfloat16)
            out[:rows, head:] = tangent.astype(jnp.bfloat16)
            pieces = split3(lse) + split3(slope_mean)
            tile = jnp.zeros((rows, head), f32)
            for at, piece in enumerate(pieces):
                tile = jnp.where(lane == at, piece, tile)
            out[rows:, :head] = tile.T[:TAIL, :].astype(jnp.bfloat16)
            out[rows:, head:] = jnp.zeros((TAIL, head), jnp.bfloat16)


def merge_kernel(own_ref, stat_ref, *refs):
    got_refs, (attended_ref, tangent_ref) = refs[:-2], refs[-2:]
    rows, head = attended_ref.shape
    f32 = jnp.float32
    parts = [(own_ref[:, :head], own_ref[:, head:], stat_ref[:, 0:1], stat_ref[:, 1:2])]
    for got in got_refs:
        cols = got[rows:, :head].astype(f32).T
        parts.append(
            (
                got[:rows, :head].astype(f32),
                got[:rows, head:].astype(f32),
                cols[:, 0:1] + cols[:, 1:2] + cols[:, 2:3],
                cols[:, 3:4] + cols[:, 4:5] + cols[:, 5:6],
            )
        )
    top = functools.reduce(jnp.maximum, [p[2] for p in parts])
    weights = [jnp.exp(p[2] - top) for p in parts]
    inverse = 1.0 / sum(weights)
    weights = [w * inverse for w in weights]
    mean = sum(w * p[3] for w, p in zip(weights, parts))
    attended_ref[...] = sum(w * p[0] for w, p in zip(weights, parts))
    tangent_ref[...] = sum(
        w * p[1] + (w * (p[3] - mean)) * p[0] for w, p in zip(weights, parts)
    )


def on_device(shape, query_rows, key_rows, value_rows, query_tangent, key_tangent, value_tangent):
    outer, inner, side, cores = shape
    plane = inner * side
    rows, head = query_rows.shape
    scale = head ** (-0.5)
    axes = ("blk", "grp")
    mix = lambda i, s, n: i ^ s if n & (n - 1) == 0 else (i + s) % n
    back = lambda i, s, n: i ^ s if n & (n - 1) == 0 else (i - s) % n

    def index(o, p, c):
        return (o * plane + p) * cores + c

    every = [(o, p, c) for o in range(outer) for p in range(plane) for c in range(cores)]
    over_plane = lambda s: [(index(o, p, c), index(o, mix(p, s, plane), c)) for o, p, c in every]
    over_core = [(index(o, p, c), index(o, p, (c + 1) % cores)) for o, p, c in every]
    over_outer = lambda s: [(index(o, p, c), index(mix(o, s, outer), p, c)) for o, p, c in every]
    outer_back = lambda s: [(index(o, p, c), index(back(o, s, outer), p, c)) for o, p, c in every]

    kv, q = pl.pallas_call(
        pack_kernel,
        out_shape=(
            jax.ShapeDtypeStruct((rows, 4 * head), key_rows.dtype),
            jax.ShapeDtypeStruct((rows, 2 * head), key_rows.dtype),
        ),
        in_specs=[pl.BlockSpec(memory_space=pltpu.HBM)] * 6,
        out_specs=(VMEM, VMEM),
        scratch_shapes=[pltpu.SemaphoreType.DMA((6,))],
        compiler_params=pltpu.CompilerParams(vmem_limit_bytes=8 * 2**20),
        name="pack",
    )(
        *(
            pltpu.with_memory_space_constraint(x, pltpu.HBM)
            for x in (key_rows, key_tangent, value_rows, value_tangent, query_rows, query_tangent)
        )
    )
    nears = [kv] + [lax.ppermute(kv, axes, over_plane(s)) for s in range(1, plane)]
    queries = [q] + [lax.ppermute(q, axes, over_outer(s)) for s in range(1, outer)]
    near = jnp.concatenate(nears, axis=0)
    far = lax.ppermute(near, axes, over_core)
    queries = jnp.concatenate(queries, axis=0)

    bf16, f32 = jnp.bfloat16, jnp.float32
    panel = pl.pallas_call(
        functools.partial(panel_kernel, outer, scale),
        out_shape=(
            jax.ShapeDtypeStruct((rows, 2 * head), f32),
            jax.ShapeDtypeStruct((rows, head), f32),
        )
        + tuple(jax.ShapeDtypeStruct((rows + TAIL, 2 * head), bf16) for _ in range(1, outer)),
        in_specs=[VMEM] * 3,
        out_specs=(VMEM,) * (1 + outer),
        compiler_params=pltpu.CompilerParams(vmem_limit_bytes=40 * 2**20),
        cost_estimate=pl.CostEstimate(
            flops=10 * queries.shape[0] * 2 * near.shape[0] * head,
            bytes_accessed=0,
            transcendentals=0,
        ),
        name="panel",
    )
    own, stat, *sends = panel(queries, near, far)
    gots = [
        lax.ppermute(block, axes, outer_back(s)) for s, block in zip(range(1, outer), sends)
    ]
    return pl.pallas_call(
        merge_kernel,
        out_shape=(jax.ShapeDtypeStruct((rows, head), f32),) * 2,
        in_specs=[VMEM] * (2 + len(gots)),
        out_specs=(VMEM, VMEM),
        compiler_params=pltpu.CompilerParams(vmem_limit_bytes=8 * 2**20),
        name="merge",
    )(own, stat, *gots)


def solution(mesh):
    blocks, group = mesh.shape["blk"], mesh.shape["grp"]
    cores = 2 if group % 2 == 0 else 1
    outer = group if blocks % group == 0 else 1
    shape = (outer, blocks // outer, group // cores, cores)
    placed = P(("blk", "grp"), None)

    def body(*args):
        return on_device(shape, *args)

    return jax.shard_map(
        body,
        mesh=mesh,
        in_specs=(placed,) * 6,
        out_specs=(placed, placed),
        check_vma=False,
    )
```

```python
import functools
import math

import jax
import jax.numpy as jnp
from jax import lax
from jax.experimental import pallas as pl
from jax.experimental.pallas import tpu as pltpu
from jax.sharding import PartitionSpec as P


TAIL = 8
VMEM = pl.BlockSpec(memory_space=pltpu.VMEM)


def pack_kernel(k, dk, v, dv, q, dq, kv_out, q_out, sems):
    head = k.shape[1]
    places = [
        (k, kv_out, 0), (dk, kv_out, 1), (v, kv_out, 2), (dv, kv_out, 3),
        (dq, q_out, 0), (q, q_out, 1),
    ]
    copies = [
        pltpu.make_async_copy(src, out.at[:, at * head : (at + 1) * head], sems.at[i])
        for i, (src, out, at) in enumerate(places)
    ]
    for copy in copies:
        copy.start()
    for copy in copies:
        copy.wait()


def split3(x):
    hi = x.astype(jnp.bfloat16).astype(jnp.float32)
    mid = (x - hi).astype(jnp.bfloat16).astype(jnp.float32)
    return hi, mid, x - hi - mid


def panel_kernel(scale, keeps, count, *refs):
    q_refs, (near_ref, far_ref), outs = refs[:count], refs[count : count + 2], refs[count + 2 :]
    rows, width = q_refs[0].shape
    head = width // 2
    nt = (((1,), (1,)), ((), ()))
    nn = (((1,), (0,)), ((), ()))
    f32 = jnp.float32
    q = jnp.concatenate([ref[...] for ref in q_refs], axis=0)
    sides = (near_ref, far_ref)
    scores = [
        lax.dot_general(q[:, head:], kv[:, :head], nt, preferred_element_type=f32) for kv in sides
    ]
    slopes = [
        lax.dot_general(q, kv[:, :width], nt, preferred_element_type=f32) for kv in sides
    ]
    top = functools.reduce(jnp.maximum, [jnp.max(s, axis=1, keepdims=True) for s in scores])
    terms = []
    for s, d, kv in zip(scores, slopes, sides):
        probs = jnp.exp2((s - top) * (scale * math.log2(math.e)))
        weighted = probs * d
        terms.append(
            (
                jnp.sum(probs, axis=1, keepdims=True),
                jnp.sum(weighted, axis=1, keepdims=True),
                lax.dot_general(
                    probs.astype(jnp.bfloat16), kv[:, width:], nn, preferred_element_type=f32
                ),
                lax.dot_general(
                    weighted.astype(jnp.bfloat16),
                    kv[:, width : width + head],
                    nn,
                    preferred_element_type=f32,
                ),
            )
        )
    total, slope_total, both, slope_part = (x + y for x, y in zip(*terms))
    inverse = 1.0 / total
    attended = both[:, :head] * inverse
    slope_mean = slope_total * (scale * inverse)
    tangent = (both[:, head:] + slope_part * scale) * inverse - slope_mean * attended
    lse = top * scale + jnp.log(total)
    lane = lax.broadcasted_iota(jnp.int32, (rows, head), 1)
    row = lax.broadcasted_iota(jnp.int32, (TAIL, head), 0)
    for block in range(count):
        at = slice(block * rows, (block + 1) * rows)
        stats = jnp.where(lane % 2 == 0, lse[at], slope_mean[at]).T[:TAIL, :]
        if keeps and block == 0:
            outs[0][:, :head], outs[0][:, head:] = attended[at], tangent[at]
            outs[1][...] = stats
            continue
        out = outs[block + 1 if keeps else block]
        out[:rows, :head] = attended[at].astype(jnp.bfloat16)
        out[:rows, head:] = tangent[at].astype(jnp.bfloat16)
        high, middle, low = split3(stats)
        out[rows:, :head] = jnp.where(row < 2, high, low).astype(jnp.bfloat16)
        out[rows:, head:] = middle.astype(jnp.bfloat16)


def merge_kernel(own_ref, stat_ref, *refs):
    got_refs, (attended_ref, tangent_ref) = refs[:-2], refs[-2:]
    rows, head = attended_ref.shape
    f32 = jnp.float32
    parts = [(own_ref[:, :head], own_ref[:, head:])]
    lse, slope = [stat_ref[0:1, :]], [stat_ref[1:2, :]]
    for got in got_refs:
        ends, middle = got[rows:, :head].astype(f32), got[rows:, head:].astype(f32)
        lse.append(ends[0:1] + middle[0:1] + ends[2:3])
        slope.append(ends[1:2] + middle[1:2] + ends[3:4])
        parts.append((got[:rows, :head].astype(f32), got[:rows, head:].astype(f32)))
    top = functools.reduce(jnp.maximum, lse)
    weights = [jnp.exp(x - top) for x in lse]
    inverse = 1.0 / sum(weights)
    weights = [w * inverse for w in weights]
    mean = sum(w * s for w, s in zip(weights, slope))
    table = jnp.concatenate(weights + [w * (s - mean) for w, s in zip(weights, slope)], axis=0)
    columns = table.T
    n = len(parts)
    shares = [columns[:, i : i + 1] for i in range(n)]
    tilts = [columns[:, n + i : n + i + 1] for i in range(n)]
    attended_ref[...] = sum(w * p[0] for w, p in zip(shares, parts))
    tangent_ref[...] = sum(w * p[1] + t * p[0] for w, t, p in zip(shares, tilts, parts))


def on_device(shape, query_rows, key_rows, value_rows, query_tangent, key_tangent, value_tangent):
    outer, inner, side, cores = shape
    plane = inner * side
    rows, head = query_rows.shape
    scale = head ** (-0.5)
    axes = ("blk", "grp")
    mix = lambda i, s, n: i ^ s if n & (n - 1) == 0 else (i + s) % n
    back = lambda i, s, n: i ^ s if n & (n - 1) == 0 else (i - s) % n

    def index(o, p, c):
        return (o * plane + p) * cores + c

    every = [(o, p, c) for o in range(outer) for p in range(plane) for c in range(cores)]
    over_plane = lambda s: [(index(o, p, c), index(o, mix(p, s, plane), c)) for o, p, c in every]
    over_core = [(index(o, p, c), index(o, p, (c + 1) % cores)) for o, p, c in every]
    over_outer = lambda s: [(index(o, p, c), index(mix(o, s, outer), p, c)) for o, p, c in every]
    outer_back = lambda s: [(index(o, p, c), index(back(o, s, outer), p, c)) for o, p, c in every]

    kv, q = pl.pallas_call(
        pack_kernel,
        out_shape=(
            jax.ShapeDtypeStruct((rows, 4 * head), key_rows.dtype),
            jax.ShapeDtypeStruct((rows, 2 * head), key_rows.dtype),
        ),
        in_specs=[pl.BlockSpec(memory_space=pltpu.HBM)] * 6,
        out_specs=(VMEM, VMEM),
        scratch_shapes=[pltpu.SemaphoreType.DMA((6,))],
        compiler_params=pltpu.CompilerParams(vmem_limit_bytes=8 * 2**20),
        name="pack",
    )(
        *(
            pltpu.with_memory_space_constraint(x, pltpu.HBM)
            for x in (key_rows, key_tangent, value_rows, value_tangent, query_rows, query_tangent)
        )
    )

    def sent(x, pairs):
        return lax.ppermute(x, axes, pairs)

    nears = [kv] + [sent(kv, over_plane(s)) for s in range(1, plane)]
    queries = [q] + [sent(q, over_outer(s)) for s in range(1, outer)]
    near = jnp.concatenate(nears, axis=0)
    far = sent(near, over_core)

    f32 = jnp.float32
    part = jax.ShapeDtypeStruct((rows + TAIL, 2 * head), jnp.bfloat16)

    def panel(which):
        keeps = 0 in which
        outs = (part,) * (len(which) - keeps)
        if keeps:
            outs = (
                jax.ShapeDtypeStruct((rows, 2 * head), f32),
                jax.ShapeDtypeStruct((TAIL, head), f32),
            ) + outs
        return pl.pallas_call(
            functools.partial(panel_kernel, scale, keeps, len(which)),
            out_shape=outs,
            in_specs=[VMEM] * (len(which) + 2),
            out_specs=(VMEM,) * len(outs),
            compiler_params=pltpu.CompilerParams(vmem_limit_bytes=40 * 2**20),
            cost_estimate=pl.CostEstimate(
                flops=20 * len(which) * rows * near.shape[0] * head,
                bytes_accessed=0,
                transcendentals=0,
            ),
        )(*(queries[i] for i in which), near, far)

    sends = {s: panel((s,))[0] for s in range(2, outer)}
    own, stat, *rest = panel(tuple(range(min(2, outer))))
    sends.update(zip((1,), rest))
    gots = [sent(sends[s], outer_back(s)) for s in range(1, outer)]
    return pl.pallas_call(
        merge_kernel,
        out_shape=(jax.ShapeDtypeStruct((rows, head), f32),) * 2,
        in_specs=[VMEM] * (2 + len(gots)),
        out_specs=(VMEM, VMEM),
        compiler_params=pltpu.CompilerParams(vmem_limit_bytes=8 * 2**20),
        name="merge",
    )(own, stat, *gots)


def solution(mesh):
    blocks, group = mesh.shape["blk"], mesh.shape["grp"]
    cores = 2 if group % 2 == 0 else 1
    outer = group if blocks % group == 0 else 1
    shape = (outer, blocks // outer, group // cores, cores)
    placed = P(("blk", "grp"), None)

    def body(*args):
        return on_device(shape, *args)

    return jax.shard_map(
        body,
        mesh=mesh,
        in_specs=(placed,) * 6,
        out_specs=(placed, placed),
        check_vma=False,
    )
```

```python
import functools
import math

import jax
import jax.numpy as jnp
from jax import lax
from jax.experimental import pallas as pl
from jax.experimental.pallas import tpu as pltpu
from jax.sharding import PartitionSpec as P


TAIL = 8
VMEM = pl.BlockSpec(memory_space=pltpu.VMEM)


def pack_kernel(k, dk, v, dv, q, dq, kv_out, q_out, sems):
    head = k.shape[1]
    places = [
        (k, kv_out, 0), (dk, kv_out, 1), (v, kv_out, 2), (dv, kv_out, 3),
        (dq, q_out, 0), (q, q_out, 1),
    ]
    copies = [
        pltpu.make_async_copy(src, out.at[:, at * head : (at + 1) * head], sems.at[i])
        for i, (src, out, at) in enumerate(places)
    ]
    for copy in copies:
        copy.start()
    for copy in copies:
        copy.wait()


def split3(x):
    hi = x.astype(jnp.bfloat16).astype(jnp.float32)
    mid = (x - hi).astype(jnp.bfloat16).astype(jnp.float32)
    return hi, mid, x - hi - mid


def panel_kernel(scale, keeps, count, sides, resumes, ends, *refs):
    q_refs, kv_refs, refs = refs[:count], refs[count : count + sides], refs[count + sides :]
    state, outs = (refs[:2], refs[2:]) if resumes else ((), refs)
    rows, width = q_refs[0].shape
    head = width // 2
    nt = (((1,), (1,)), ((), ()))
    nn = (((1,), (0,)), ((), ()))
    f32 = jnp.float32
    step = scale * math.log2(math.e)
    q = jnp.concatenate([ref[...] for ref in q_refs], axis=0)
    scores = [
        lax.dot_general(q[:, head:], kv[:, :head], nt, preferred_element_type=f32)
        for kv in kv_refs
    ]
    slopes = [
        lax.dot_general(q, kv[:, :width], nt, preferred_element_type=f32) for kv in kv_refs
    ]
    tile = (q.shape[0], head)
    over = lambda x, wide: jnp.concatenate([x] * (wide // head), axis=1)
    tops = [
        jnp.broadcast_to(jnp.max(s, axis=1, keepdims=True), tile) for s in scores
    ]
    if resumes:
        sums_ref, lines_ref = state
        tops.append(lines_ref[:, :head])
    top = functools.reduce(jnp.maximum, tops)
    terms = []
    if resumes:
        fade = jnp.exp2((tops[-1] - top) * step)
        terms.append(
            (
                lines_ref[:, head:width] * fade,
                lines_ref[:, width:] * fade,
                sums_ref[:, :width] * over(fade, width),
                sums_ref[:, width:] * fade,
            )
        )
    for s, d, kv in zip(scores, slopes, kv_refs):
        probs = jnp.exp2((s - over(top, s.shape[1])) * step)
        weighted = probs * d
        terms.append(
            (
                jnp.broadcast_to(jnp.sum(probs, axis=1, keepdims=True), tile),
                jnp.broadcast_to(jnp.sum(weighted, axis=1, keepdims=True), tile),
                lax.dot_general(
                    probs.astype(jnp.bfloat16), kv[:, width:], nn, preferred_element_type=f32
                ),
                lax.dot_general(
                    weighted.astype(jnp.bfloat16),
                    kv[:, width : width + head],
                    nn,
                    preferred_element_type=f32,
                ),
            )
        )
    total, slope_total, both, slope_part = (functools.reduce(jnp.add, x) for x in zip(*terms))
    if not ends:
        sums_ref, lines_ref = outs
        sums_ref[:, :width], sums_ref[:, width:] = both, slope_part
        lines_ref[...] = jnp.concatenate([top, total, slope_total], axis=1)
        return
    inverse = 1.0 / total
    attended = both[:, :head] * inverse
    slope_mean = slope_total * (scale * inverse)
    tangent = (both[:, head:] + slope_part * scale) * inverse - slope_mean * attended
    lse = top * scale + jnp.log(total)
    lane = lax.broadcasted_iota(jnp.int32, (rows, head), 1)
    row = lax.broadcasted_iota(jnp.int32, (TAIL, head), 0)
    for block in range(count):
        at = slice(block * rows, (block + 1) * rows)
        stats = jnp.where(lane % 2 == 0, lse[at], slope_mean[at]).T[:TAIL, :]
        if keeps and block == 0:
            outs[0][:, :head], outs[0][:, head:] = attended[at], tangent[at]
            outs[1][...] = stats
            continue
        out = outs[block + 1 if keeps else block]
        out[:rows, :head] = attended[at].astype(jnp.bfloat16)
        out[:rows, head:] = tangent[at].astype(jnp.bfloat16)
        high, middle, low = split3(stats)
        out[rows:, :head] = jnp.where(row < 2, high, low).astype(jnp.bfloat16)
        out[rows:, head:] = middle.astype(jnp.bfloat16)


def merge_kernel(own_ref, stat_ref, *refs):
    got_refs, (attended_ref, tangent_ref) = refs[:-2], refs[-2:]
    rows, head = attended_ref.shape
    f32 = jnp.float32
    parts = [(own_ref[:, :head], own_ref[:, head:])]
    lse, slope = [stat_ref[0:1, :]], [stat_ref[1:2, :]]
    for got in got_refs:
        ends, middle = got[rows:, :head].astype(f32), got[rows:, head:].astype(f32)
        lse.append(ends[0:1] + middle[0:1] + ends[2:3])
        slope.append(ends[1:2] + middle[1:2] + ends[3:4])
        parts.append((got[:rows, :head].astype(f32), got[:rows, head:].astype(f32)))
    top = functools.reduce(jnp.maximum, lse)
    weights = [jnp.exp(x - top) for x in lse]
    inverse = 1.0 / sum(weights)
    weights = [w * inverse for w in weights]
    mean = sum(w * s for w, s in zip(weights, slope))
    table = jnp.concatenate(weights + [w * (s - mean) for w, s in zip(weights, slope)], axis=0)
    columns = table.T
    n = len(parts)
    shares = [columns[:, i : i + 1] for i in range(n)]
    tilts = [columns[:, n + i : n + i + 1] for i in range(n)]
    attended_ref[...] = sum(w * p[0] for w, p in zip(shares, parts))
    tangent_ref[...] = sum(w * p[1] + t * p[0] for w, t, p in zip(shares, tilts, parts))


def on_device(shape, query_rows, key_rows, value_rows, query_tangent, key_tangent, value_tangent):
    outer, inner, side, cores = shape
    plane = inner * side
    rows, head = query_rows.shape
    scale = head ** (-0.5)
    axes = ("blk", "grp")
    mix = lambda i, s, n: i ^ s if n & (n - 1) == 0 else (i + s) % n

    def index(o, p, c):
        return (o * plane + p) * cores + c

    every = [(o, p, c) for o in range(outer) for p in range(plane) for c in range(cores)]
    over_plane = lambda s: [(index(o, p, c), index(o, mix(p, s, plane), c)) for o, p, c in every]
    over_core = [(index(o, p, c), index(o, p, (c + 1) % cores)) for o, p, c in every]
    over_outer = lambda s: [(index(o, p, c), index((o + s) % outer, p, c)) for o, p, c in every]
    outer_back = lambda s: over_outer(outer - s)

    kv, q = pl.pallas_call(
        pack_kernel,
        out_shape=(
            jax.ShapeDtypeStruct((rows, 4 * head), key_rows.dtype),
            jax.ShapeDtypeStruct((rows, 2 * head), key_rows.dtype),
        ),
        in_specs=[pl.BlockSpec(memory_space=pltpu.HBM)] * 6,
        out_specs=(VMEM, VMEM),
        scratch_shapes=[pltpu.SemaphoreType.DMA((6,))],
        compiler_params=pltpu.CompilerParams(vmem_limit_bytes=8 * 2**20),
        name="pack",
    )(
        *(
            pltpu.with_memory_space_constraint(x, pltpu.HBM)
            for x in (key_rows, key_tangent, value_rows, value_tangent, query_rows, query_tangent)
        )
    )

    def sent(x, pairs):
        return lax.ppermute(x, axes, pairs)

    nears = [kv] + [sent(kv, over_plane(s)) for s in range(1, plane)]
    queries = [q] + [sent(q, over_outer(s)) for s in range(1, outer)]
    first = jnp.concatenate(nears[:-1], axis=0)
    early = (first, sent(first, over_core))
    late = (nears[-1], sent(nears[-1], over_core))

    f32 = jnp.float32
    part = jax.ShapeDtypeStruct((rows + TAIL, 2 * head), jnp.bfloat16)

    def panel(which, sides, resumes=(), ends=True):
        keeps = ends and 0 in which
        n = len(which)
        if not ends:
            outs = (
                jax.ShapeDtypeStruct((n * rows, 3 * head), f32),
                jax.ShapeDtypeStruct((n * rows, 3 * head), f32),
            )
        elif keeps:
            outs = (
                jax.ShapeDtypeStruct((rows, 2 * head), f32),
                jax.ShapeDtypeStruct((TAIL, head), f32),
            ) + (part,) * (n - 1)
        else:
            outs = (part,) * n
        keys = sum(kv.shape[0] for kv in sides)
        return pl.pallas_call(
            functools.partial(
                panel_kernel, scale, keeps, n, len(sides), bool(resumes), ends
            ),
            out_shape=outs,
            in_specs=[VMEM] * (n + len(sides) + len(resumes)),
            out_specs=(VMEM,) * len(outs),
            compiler_params=pltpu.CompilerParams(vmem_limit_bytes=40 * 2**20),
            cost_estimate=pl.CostEstimate(
                flops=20 * n * rows * keys * head, bytes_accessed=0, transcendentals=0
            ),
        )(*(queries[i] for i in which), *sides, *resumes)

    remote = tuple(range(2, outer))
    state = panel(remote, early, ends=False)
    sends = dict(zip(remote, panel(remote, late, state)))
    own, stat, sends[1] = panel((0, 1), early + late)
    gots = [sent(sends[s], outer_back(s)) for s in range(1, outer)]
    return pl.pallas_call(
        merge_kernel,
        out_shape=(jax.ShapeDtypeStruct((rows, head), f32),) * 2,
        in_specs=[VMEM] * (2 + len(gots)),
        out_specs=(VMEM, VMEM),
        compiler_params=pltpu.CompilerParams(vmem_limit_bytes=8 * 2**20),
        name="merge",
    )(own, stat, *gots)


def solution(mesh):
    blocks, group = mesh.shape["blk"], mesh.shape["grp"]
    cores = 2 if group % 2 == 0 else 1
    outer = group if blocks % group == 0 else 1
    shape = (outer, blocks // outer, group // cores, cores)
    placed = P(("blk", "grp"), None)

    def body(*args):
        return on_device(shape, *args)

    return jax.shard_map(
        body,
        mesh=mesh,
        in_specs=(placed,) * 6,
        out_specs=(placed, placed),
        check_vma=False,
    )
```

```python
import functools
import math

import jax
import jax.numpy as jnp
from jax import lax
from jax.experimental import pallas as pl
from jax.experimental.pallas import tpu as pltpu
from jax.sharding import PartitionSpec as P


TAIL = 8
VMEM = pl.BlockSpec(memory_space=pltpu.VMEM)


def pack_kernel(k, dk, v, dv, q, dq, kv_out, q_out, sems):
    head = k.shape[1]
    places = [
        (k, kv_out, 0), (dk, kv_out, 1), (v, kv_out, 2), (dv, kv_out, 3),
        (dq, q_out, 0), (q, q_out, 1),
    ]
    copies = [
        pltpu.make_async_copy(src, out.at[:, at * head : (at + 1) * head], sems.at[i])
        for i, (src, out, at) in enumerate(places)
    ]
    for copy in copies:
        copy.start()
    for copy in copies:
        copy.wait()


def split3(x):
    hi = x.astype(jnp.bfloat16).astype(jnp.float32)
    mid = (x - hi).astype(jnp.bfloat16).astype(jnp.float32)
    return hi, mid, x - hi - mid


def panel_kernel(scale, keeps, count, sides, resumes, ends, *refs):
    q_refs, kv_refs, refs = refs[:count], refs[count : count + sides], refs[count + sides :]
    state, outs = (refs[:2], refs[2:]) if resumes else ((), refs)
    rows, width = q_refs[0].shape
    head = width // 2
    nt = (((1,), (1,)), ((), ()))
    nn = (((1,), (0,)), ((), ()))
    f32 = jnp.float32
    step = scale * math.log2(math.e)
    q = jnp.concatenate([ref[...] for ref in q_refs], axis=0)
    scores = [
        lax.dot_general(q[:, head:], kv[:, :head], nt, preferred_element_type=f32)
        for kv in kv_refs
    ]
    slopes = [
        lax.dot_general(q, kv[:, :width], nt, preferred_element_type=f32) for kv in kv_refs
    ]
    tile = (q.shape[0], head)
    over = lambda x, wide: jnp.concatenate([x] * (wide // head), axis=1)
    tops = [
        jnp.broadcast_to(jnp.max(s, axis=1, keepdims=True), tile) for s in scores
    ]
    if resumes:
        sums_ref, lines_ref = state
        tops.append(lines_ref[:, :head])
    top = functools.reduce(jnp.maximum, tops)
    terms = []
    if resumes:
        fade = jnp.exp2((tops[-1] - top) * step)
        terms.append(
            (
                lines_ref[:, head:width] * fade,
                lines_ref[:, width:] * fade,
                sums_ref[:, :width] * over(fade, width),
                sums_ref[:, width:] * fade,
            )
        )
    for s, d, kv in zip(scores, slopes, kv_refs):
        probs = jnp.exp2((s - over(top, s.shape[1])) * step)
        weighted = probs * d
        terms.append(
            (
                jnp.broadcast_to(jnp.sum(probs, axis=1, keepdims=True), tile),
                jnp.broadcast_to(jnp.sum(weighted, axis=1, keepdims=True), tile),
                lax.dot_general(
                    probs.astype(jnp.bfloat16), kv[:, width:], nn, preferred_element_type=f32
                ),
                lax.dot_general(
                    weighted.astype(jnp.bfloat16),
                    kv[:, width : width + head],
                    nn,
                    preferred_element_type=f32,
                ),
            )
        )
    total, slope_total, both, slope_part = (functools.reduce(jnp.add, x) for x in zip(*terms))
    if not ends:
        sums_ref, lines_ref = outs
        sums_ref[:, :width], sums_ref[:, width:] = both, slope_part
        lines_ref[...] = jnp.concatenate([top, total, slope_total], axis=1)
        return
    inverse = 1.0 / total
    attended = both[:, :head] * inverse
    slope_mean = slope_total * (scale * inverse)
    tangent = (both[:, head:] + slope_part * scale) * inverse - slope_mean * attended
    lse = top * scale + jnp.log(total)
    lane = lax.broadcasted_iota(jnp.int32, (rows, head), 1)
    row = lax.broadcasted_iota(jnp.int32, (TAIL, head), 0)
    for block in range(count):
        at = slice(block * rows, (block + 1) * rows)
        stats = jnp.where(lane % 2 == 0, lse[at], slope_mean[at]).T[:TAIL, :]
        if keeps and block == 0:
            outs[0][:, :head], outs[0][:, head:] = attended[at], tangent[at]
            outs[1][...] = stats
            continue
        out = outs[block + 1 if keeps else block]
        out[:rows, :head] = attended[at].astype(jnp.bfloat16)
        out[:rows, head:] = tangent[at].astype(jnp.bfloat16)
        high, middle, low = split3(stats)
        out[rows:, :head] = jnp.where(row < 2, high, low).astype(jnp.bfloat16)
        out[rows:, head:] = middle.astype(jnp.bfloat16)


def merge_kernel(own_ref, stat_ref, *refs):
    got_refs, (attended_ref, tangent_ref) = refs[:-2], refs[-2:]
    rows, head = attended_ref.shape
    f32 = jnp.float32
    parts = [(own_ref[:, :head], own_ref[:, head:])]
    lse, slope = [stat_ref[0:1, :]], [stat_ref[1:2, :]]
    for got in got_refs:
        ends, middle = got[rows:, :head].astype(f32), got[rows:, head:].astype(f32)
        lse.append(ends[0:1] + middle[0:1] + ends[2:3])
        slope.append(ends[1:2] + middle[1:2] + ends[3:4])
        parts.append((got[:rows, :head].astype(f32), got[:rows, head:].astype(f32)))
    top = functools.reduce(jnp.maximum, lse)
    weights = [jnp.exp(x - top) for x in lse]
    inverse = 1.0 / sum(weights)
    weights = [w * inverse for w in weights]
    mean = sum(w * s for w, s in zip(weights, slope))
    table = jnp.concatenate(weights + [w * (s - mean) for w, s in zip(weights, slope)], axis=0)
    columns = table.T
    n = len(parts)
    shares = [columns[:, i : i + 1] for i in range(n)]
    tilts = [columns[:, n + i : n + i + 1] for i in range(n)]
    attended_ref[...] = sum(w * p[0] for w, p in zip(shares, parts))
    tangent_ref[...] = sum(w * p[1] + t * p[0] for w, t, p in zip(shares, tilts, parts))


def on_device(shape, query_rows, key_rows, value_rows, query_tangent, key_tangent, value_tangent):
    outer, inner, side, cores = shape
    plane = inner * side
    rows, head = query_rows.shape
    scale = head ** (-0.5)
    axes = ("blk", "grp")
    mix = lambda i, s, n: i ^ s if n & (n - 1) == 0 else (i + s) % n

    def index(o, p, c):
        return (o * plane + p) * cores + c

    every = [(o, p, c) for o in range(outer) for p in range(plane) for c in range(cores)]
    over_plane = lambda s: [(index(o, p, c), index(o, mix(p, s, plane), c)) for o, p, c in every]
    over_core = [(index(o, p, c), index(o, p, (c + 1) % cores)) for o, p, c in every]
    over_outer = lambda s: [(index(o, p, c), index((o + s) % outer, p, c)) for o, p, c in every]
    outer_back = lambda s: over_outer(outer - s)

    kv, q = pl.pallas_call(
        pack_kernel,
        out_shape=(
            jax.ShapeDtypeStruct((rows, 4 * head), key_rows.dtype),
            jax.ShapeDtypeStruct((rows, 2 * head), key_rows.dtype),
        ),
        in_specs=[pl.BlockSpec(memory_space=pltpu.HBM)] * 6,
        out_specs=(VMEM, VMEM),
        scratch_shapes=[pltpu.SemaphoreType.DMA((6,))],
        compiler_params=pltpu.CompilerParams(vmem_limit_bytes=8 * 2**20),
        name="pack",
    )(
        *(
            pltpu.with_memory_space_constraint(x, pltpu.HBM)
            for x in (key_rows, key_tangent, value_rows, value_tangent, query_rows, query_tangent)
        )
    )

    def sent(x, pairs):
        return lax.ppermute(x, axes, pairs)

    nears = [kv] + [sent(kv, over_plane(s)) for s in range(1, plane)]
    queries = [q] + [sent(q, over_outer(s)) for s in range(1, outer)]
    halves = [
        jnp.concatenate(x, axis=0) for x in (nears[: plane // 2], nears[plane // 2 :])
    ]
    early = (halves[0], sent(halves[0], over_core))
    late = (halves[1], sent(halves[1], over_core))

    f32 = jnp.float32
    part = jax.ShapeDtypeStruct((rows + TAIL, 2 * head), jnp.bfloat16)

    def panel(which, sides, resumes=(), ends=True):
        keeps = ends and 0 in which
        n = len(which)
        if not ends:
            outs = (
                jax.ShapeDtypeStruct((n * rows, 3 * head), f32),
                jax.ShapeDtypeStruct((n * rows, 3 * head), f32),
            )
        elif keeps:
            outs = (
                jax.ShapeDtypeStruct((rows, 2 * head), f32),
                jax.ShapeDtypeStruct((TAIL, head), f32),
            ) + (part,) * (n - 1)
        else:
            outs = (part,) * n
        keys = sum(kv.shape[0] for kv in sides)
        return pl.pallas_call(
            functools.partial(
                panel_kernel, scale, keeps, n, len(sides), bool(resumes), ends
            ),
            out_shape=outs,
            in_specs=[VMEM] * (n + len(sides) + len(resumes)),
            out_specs=(VMEM,) * len(outs),
            compiler_params=pltpu.CompilerParams(vmem_limit_bytes=40 * 2**20),
            cost_estimate=pl.CostEstimate(
                flops=20 * n * rows * keys * head, bytes_accessed=0, transcendentals=0
            ),
        )(*(queries[i] for i in which), *sides, *resumes)

    remote = tuple(range(2, outer))
    state = panel(remote, early, ends=False)
    sends = dict(zip(remote, panel(remote, late, state)))
    own, stat, sends[1] = panel((0, 1), early + late)
    gots = [sent(sends[s], outer_back(s)) for s in range(1, outer)]
    return pl.pallas_call(
        merge_kernel,
        out_shape=(jax.ShapeDtypeStruct((rows, head), f32),) * 2,
        in_specs=[VMEM] * (2 + len(gots)),
        out_specs=(VMEM, VMEM),
        compiler_params=pltpu.CompilerParams(vmem_limit_bytes=8 * 2**20),
        name="merge",
    )(own, stat, *gots)


def solution(mesh):
    blocks, group = mesh.shape["blk"], mesh.shape["grp"]
    cores = 2 if group % 2 == 0 else 1
    outer = group if blocks % group == 0 else 1
    shape = (outer, blocks // outer, group // cores, cores)
    placed = P(("blk", "grp"), None)

    def body(*args):
        return on_device(shape, *args)

    return jax.shard_map(
        body,
        mesh=mesh,
        in_specs=(placed,) * 6,
        out_specs=(placed, placed),
        check_vma=False,
    )
```

```python
import functools
import math

import jax
import jax.numpy as jnp
from jax import lax
from jax.experimental import pallas as pl
from jax.experimental.pallas import tpu as pltpu
from jax.sharding import PartitionSpec as P


TAIL = 8
VMEM = pl.BlockSpec(memory_space=pltpu.VMEM)


def pack_kernel(k, dk, v, dv, q, dq, kv_out, q_out, sems):
    head = k.shape[1]
    places = [
        (k, kv_out, 0), (dk, kv_out, 1), (v, kv_out, 2), (dv, kv_out, 3),
        (dq, q_out, 0), (q, q_out, 1),
    ]
    copies = [
        pltpu.make_async_copy(src, out.at[:, at * head : (at + 1) * head], sems.at[i])
        for i, (src, out, at) in enumerate(places)
    ]
    for copy in copies:
        copy.start()
    for copy in copies:
        copy.wait()


def split3(x):
    hi = x.astype(jnp.bfloat16).astype(jnp.float32)
    mid = (x - hi).astype(jnp.bfloat16).astype(jnp.float32)
    return hi, mid, x - hi - mid


def panel_kernel(scale, keeps, count, sides, resumes, ends, *refs):
    q_refs, kv_refs, refs = refs[:count], refs[count : count + sides], refs[count + sides :]
    state, outs = (refs[:2], refs[2:]) if resumes else ((), refs)
    rows, width = q_refs[0].shape
    head = width // 2
    nt = (((1,), (1,)), ((), ()))
    nn = (((1,), (0,)), ((), ()))
    f32 = jnp.float32
    step = scale * math.log2(math.e)
    q = jnp.concatenate([ref[...] for ref in q_refs], axis=0)
    scores = [
        lax.dot_general(q[:, head:], kv[:, :head], nt, preferred_element_type=f32)
        for kv in kv_refs
    ]
    slopes = [
        lax.dot_general(q, kv[:, :width], nt, preferred_element_type=f32) for kv in kv_refs
    ]
    tile = (q.shape[0], head)
    over = lambda x, wide: jnp.concatenate([x] * (wide // head), axis=1)
    tops = [
        jnp.broadcast_to(jnp.max(s, axis=1, keepdims=True), tile) for s in scores
    ]
    if resumes:
        sums_ref, lines_ref = state
        tops.append(lines_ref[:, :head])
    top = functools.reduce(jnp.maximum, tops)
    terms = []
    if resumes:
        fade = jnp.exp2((tops[-1] - top) * step)
        terms.append(
            (
                lines_ref[:, head:width] * fade,
                lines_ref[:, width:] * fade,
                sums_ref[:, :width] * over(fade, width),
                sums_ref[:, width:] * fade,
            )
        )
    for s, d, kv in zip(scores, slopes, kv_refs):
        probs = jnp.exp2((s - over(top, s.shape[1])) * step)
        weighted = probs * d
        terms.append(
            (
                jnp.broadcast_to(jnp.sum(probs, axis=1, keepdims=True), tile),
                jnp.broadcast_to(jnp.sum(weighted, axis=1, keepdims=True), tile),
                lax.dot_general(
                    probs.astype(jnp.bfloat16), kv[:, width:], nn, preferred_element_type=f32
                ),
                lax.dot_general(
                    weighted.astype(jnp.bfloat16),
                    kv[:, width : width + head],
                    nn,
                    preferred_element_type=f32,
                ),
            )
        )
    total, slope_total, both, slope_part = (functools.reduce(jnp.add, x) for x in zip(*terms))
    if not ends:
        sums_ref, lines_ref = outs
        sums_ref[:, :width], sums_ref[:, width:] = both, slope_part
        lines_ref[...] = jnp.concatenate([top, total, slope_total], axis=1)
        return
    inverse = 1.0 / total
    attended = both[:, :head] * inverse
    slope_mean = slope_total * (scale * inverse)
    tangent = (both[:, head:] + slope_part * scale) * inverse - slope_mean * attended
    lse = top * scale + jnp.log(total)
    lane = lax.broadcasted_iota(jnp.int32, (rows, head), 1)
    row = lax.broadcasted_iota(jnp.int32, (TAIL, head), 0)
    for block in range(count):
        at = slice(block * rows, (block + 1) * rows)
        stats = jnp.where(lane % 2 == 0, lse[at], slope_mean[at]).T[:TAIL, :]
        if keeps and block == 0:
            outs[0][:, :head], outs[0][:, head:] = attended[at], tangent[at]
            outs[1][...] = stats
            continue
        out = outs[block + 1 if keeps else block]
        out[:rows, :head] = attended[at].astype(jnp.bfloat16)
        out[:rows, head:] = tangent[at].astype(jnp.bfloat16)
        high, middle, low = split3(stats)
        out[rows:, :head] = jnp.where(row < 2, high, low).astype(jnp.bfloat16)
        out[rows:, head:] = middle.astype(jnp.bfloat16)


def merge_kernel(own_ref, stat_ref, *refs):
    got_refs, (attended_ref, tangent_ref) = refs[:-2], refs[-2:]
    rows, head = attended_ref.shape
    f32 = jnp.float32
    parts = [(own_ref[:, :head], own_ref[:, head:])]
    lse, slope = [stat_ref[0:1, :]], [stat_ref[1:2, :]]
    for got in got_refs:
        ends, middle = got[rows:, :head].astype(f32), got[rows:, head:].astype(f32)
        lse.append(ends[0:1] + middle[0:1] + ends[2:3])
        slope.append(ends[1:2] + middle[1:2] + ends[3:4])
        parts.append((got[:rows, :head].astype(f32), got[:rows, head:].astype(f32)))
    top = functools.reduce(jnp.maximum, lse)
    weights = [jnp.exp(x - top) for x in lse]
    inverse = 1.0 / sum(weights)
    weights = [w * inverse for w in weights]
    mean = sum(w * s for w, s in zip(weights, slope))
    table = jnp.concatenate(weights + [w * (s - mean) for w, s in zip(weights, slope)], axis=0)
    columns = table.T
    n = len(parts)
    shares = [columns[:, i : i + 1] for i in range(n)]
    tilts = [columns[:, n + i : n + i + 1] for i in range(n)]
    attended_ref[...] = sum(w * p[0] for w, p in zip(shares, parts))
    tangent_ref[...] = sum(w * p[1] + t * p[0] for w, t, p in zip(shares, tilts, parts))


def on_device(shape, query_rows, key_rows, value_rows, query_tangent, key_tangent, value_tangent):
    outer, inner, side, cores = shape
    plane = inner * side
    rows, head = query_rows.shape
    scale = head ** (-0.5)
    axes = ("blk", "grp")
    mix = lambda i, s, n: i ^ s if n & (n - 1) == 0 else (i + s) % n

    def index(o, p, c):
        return (o * plane + p) * cores + c

    every = [(o, p, c) for o in range(outer) for p in range(plane) for c in range(cores)]
    turn = lambda s, c: 1 + (s - 1 + c) % (plane - 1)
    over_plane = lambda s: [
        (index(o, p, c), index(o, mix(p, turn(s, c), plane), c)) for o, p, c in every
    ]
    over_core = [(index(o, p, c), index(o, p, (c + 1) % cores)) for o, p, c in every]
    over_outer = lambda s: [(index(o, p, c), index((o + s) % outer, p, c)) for o, p, c in every]
    outer_back = lambda s: over_outer(outer - s)

    kv, q = pl.pallas_call(
        pack_kernel,
        out_shape=(
            jax.ShapeDtypeStruct((rows, 4 * head), key_rows.dtype),
            jax.ShapeDtypeStruct((rows, 2 * head), key_rows.dtype),
        ),
        in_specs=[pl.BlockSpec(memory_space=pltpu.HBM)] * 6,
        out_specs=(VMEM, VMEM),
        scratch_shapes=[pltpu.SemaphoreType.DMA((6,))],
        compiler_params=pltpu.CompilerParams(vmem_limit_bytes=8 * 2**20),
        name="pack",
    )(
        *(
            pltpu.with_memory_space_constraint(x, pltpu.HBM)
            for x in (key_rows, key_tangent, value_rows, value_tangent, query_rows, query_tangent)
        )
    )

    def sent(x, pairs):
        return lax.ppermute(x, axes, pairs)

    nears = [kv] + [sent(kv, over_plane(s)) for s in range(1, plane)]
    queries = [q] + [sent(q, over_outer(s)) for s in range(1, outer)]
    first = jnp.concatenate(nears[:-1], axis=0)
    early = (first, sent(first, over_core))
    late = (nears[-1], sent(nears[-1], over_core))

    f32 = jnp.float32
    part = jax.ShapeDtypeStruct((rows + TAIL, 2 * head), jnp.bfloat16)

    def panel(which, sides, resumes=(), ends=True):
        keeps = ends and 0 in which
        n = len(which)
        if not ends:
            outs = (
                jax.ShapeDtypeStruct((n * rows, 3 * head), f32),
                jax.ShapeDtypeStruct((n * rows, 3 * head), f32),
            )
        elif keeps:
            outs = (
                jax.ShapeDtypeStruct((rows, 2 * head), f32),
                jax.ShapeDtypeStruct((TAIL, head), f32),
            ) + (part,) * (n - 1)
        else:
            outs = (part,) * n
        keys = sum(kv.shape[0] for kv in sides)
        return pl.pallas_call(
            functools.partial(
                panel_kernel, scale, keeps, n, len(sides), bool(resumes), ends
            ),
            out_shape=outs,
            in_specs=[VMEM] * (n + len(sides) + len(resumes)),
            out_specs=(VMEM,) * len(outs),
            compiler_params=pltpu.CompilerParams(vmem_limit_bytes=40 * 2**20),
            cost_estimate=pl.CostEstimate(
                flops=20 * n * rows * keys * head, bytes_accessed=0, transcendentals=0
            ),
        )(*(queries[i] for i in which), *sides, *resumes)

    remote = tuple(range(2, outer))
    state = panel(remote, early, ends=False)
    sends = dict(zip(remote, panel(remote, late, state)))
    own, stat, sends[1] = panel((0, 1), early + late)
    gots = [sent(sends[s], outer_back(s)) for s in range(1, outer)]
    return pl.pallas_call(
        merge_kernel,
        out_shape=(jax.ShapeDtypeStruct((rows, head), f32),) * 2,
        in_specs=[VMEM] * (2 + len(gots)),
        out_specs=(VMEM, VMEM),
        compiler_params=pltpu.CompilerParams(vmem_limit_bytes=8 * 2**20),
        name="merge",
    )(own, stat, *gots)


def solution(mesh):
    blocks, group = mesh.shape["blk"], mesh.shape["grp"]
    cores = 2 if group % 2 == 0 else 1
    outer = group if blocks % group == 0 else 1
    shape = (outer, blocks // outer, group // cores, cores)
    placed = P(("blk", "grp"), None)

    def body(*args):
        return on_device(shape, *args)

    return jax.shard_map(
        body,
        mesh=mesh,
        in_specs=(placed,) * 6,
        out_specs=(placed, placed),
        check_vma=False,
    )
```
